32 devices in a mesh: owner: 8 (over z, y), rows: 4 (over x, core).
Axes of the slice: x: 2, y: 2, z: 4, core: 2. Of those that a mesh axis runs over, the one named last changes fastest.
Arguments:
- master_down: float32 [16, 6400, 4096], P('owner', None, 'rows'), may hold values from -0.109375 to 0.109375
- router_weight: float32 [4096, 16], P('rows', 'owner'), may hold values from -0.09375 to 0.09375
- router_gain: float32 [4096], P('rows'), may hold values from 0.25 to 1.75
Outputs:
- final_down: bfloat16 [16, 6400, 4096], P('owner', 'rows')
- scale_down: float32 [16, 6400], P('owner', 'rows')
- serve_router: bfloat16 [4096, 16], replicated
The draws below stay inside these ranges and needn't reach their ends.
All inputs are finite; a program needn't handle non-finite values. Where the reference program divides by a largest or mean magnitude, that divisor is 1e-20 or more.
Results may differ from the reference program's by a relative error of at most 0.001.
Values may be sent and summed in bfloat16 or wider, within the bound.
No kernel may reach another device: no remote copies, remote signals or barrier semaphores. Data moves between devices by JAX's collectives and lax.ppermute only.
A program may use at most 192 MiB of HBM per device.

```python
import jax
import jax.numpy as jnp

EXPERTS = 16
D_MODEL = 4096
D_EXPERT = 6400


def with_spikes(entries, rng, source, target, blocks, factor):
    owner, partner = [(jnp.arange(entries.shape[position]) // (entries.shape[position] // blocks)).reshape([-1 if axis == position else 1 for axis in range(entries.ndim)]) for position in (source, target)]
    chosen = jax.random.permutation(rng, blocks)[partner]
    strong = (owner == chosen) | (owner == (partner + blocks // 2) % blocks)
    return jnp.where(strong, factor * entries, entries)


def level_of(key, dims, cuts, low, largest):
    def one(axis_at, shards_of):
        heights = jax.random.uniform(jax.random.fold_in(jax.random.fold_in(key, 6), axis_at), (shards_of,), jnp.float32, low / len(cuts), largest / len(cuts))
        return jnp.repeat(jnp.exp(heights), dims[axis_at] // shards_of).reshape((-1,) + (1,) * (len(dims) - axis_at - 1))

    level = one(*cuts[0])
    for cut in cuts[1:]:
        level = level * one(*cut)
    return level


def gaussian(own_key, extent, deviation, bound, shards=(), dtype=jnp.bfloat16):
    drawn = deviation * jax.random.normal(own_key, extent, jnp.float32)
    if shards:
        drawn = drawn * level_of(own_key, extent, shards, -0.22, 0.18)
    return jnp.clip(drawn, -bound, bound).astype(dtype)


def heavy_noise(rng, dims, spread, bound, split, heavy, held_as=jnp.bfloat16):
    entries = spread * jax.random.normal(rng, dims, jnp.float32)
    if split:
        entries = entries * level_of(rng, dims, split, -0.22, 0.18)
    return jnp.clip(with_spikes(entries, jax.random.fold_in(rng, 3), *heavy), -bound, bound).astype(held_as)


def setup_inputs(seed: int = 0) -> dict:
    key_list = jax.random.split(jax.random.key(seed), 4)
    return {
        "master_down": heavy_noise(key_list[0], (EXPERTS, D_EXPERT, D_MODEL), D_EXPERT ** -0.5, 0.109375, ((0, 8), (2, 4)), (2, 1, 4, 2.0), jnp.float32),
        "router_weight": gaussian(key_list[1], (D_MODEL, EXPERTS), D_MODEL ** -0.5, 0.09375, ((0, 4), (1, 8)), jnp.float32),
        "router_gain": jnp.clip(1.0 + 0.15 * jax.random.normal(key_list[2], (D_MODEL,), jnp.float32), 0.25, 1.75),
    }


def reference(master_down, router_weight, router_gain):
    scale_down = jnp.sum(jnp.abs(master_down), axis=2) / D_MODEL
    final_down = (master_down / jnp.expand_dims(scale_down, 2)).astype(jnp.bfloat16)
    serve_router = (router_weight * router_gain[:, None]).astype(jnp.bfloat16)
    return final_down, scale_down, serve_router
```

```python
import jax
import jax.numpy as jnp
from jax import lax
from jax.experimental import pallas as pl
from jax.experimental.pallas import tpu as pltpu
from jax.sharding import PartitionSpec as P


LANES, TILE = 128, 16
GROUPS = ((2, 2), (4, 4, 4), (5, 5, 5, 5, 5, 4, 3, 2))
AHEAD = 4
ROUTER_SENT, ROUTER_USED = 3, 7


def plan(rows):
    total, at, done, groups = sum(map(sum, GROUPS)), 0, 0, []
    for lengths in GROUPS:
        chunks = []
        for length in lengths:
            done += length
            end = rows if done == total else rows * done // total // TILE * TILE
            if end > at:
                chunks.append((at, end - at))
            at = end
        if chunks:
            groups.append(chunks)
    return groups


def block_of(first, count):
    return max((u for u in range(TILE, 81, TILE) if first % u == 0 and count % u == 0), default=count)


def tree_sum(terms):
    terms = list(terms)
    while len(terms) > 1:
        terms = [sum(terms[i + 1 : i + 2], terms[i]) for i in range(0, len(terms), 2)]
    return terms[0]


def narrow(out, blocks, sums, base, places, first, count, after):
    experts, n, rows, width = blocks.shape
    model = n * width
    step = block_of(first, count)

    def body(places_ref, *refs):
        ins, sums_refs = refs[:n], refs[n : 2 * n]
        outs, factors = refs[-n - 1 : -1], refs[-1]
        e, i = pl.program_id(0), pl.program_id(1)

        @pl.when(i == 0)
        def _():
            inverse = 1.0 / (tree_sum(r[e, :, first - base : first - base + count] for r in sums_refs) / model)
            row = lax.broadcasted_iota(jnp.int32, inverse.shape, 0)
            for k in range(n):
                chosen = jnp.sum(jnp.where(row == places_ref[k], inverse, 0.0), axis=0, keepdims=True)
                factors[k] = jnp.broadcast_to(chosen, (LANES, count)).T

        rows_now = pl.ds(pl.multiple_of(i * step, step), step)
        for k in range(n):
            factor = factors[k, rows_now, :]
            for j in range(0, width, LANES):
                outs[k][0, :, j : j + LANES] = (ins[k][0, 0, :, j : j + LANES] * factor).astype(jnp.bfloat16)

    def reader(k):
        return pl.BlockSpec((1, 1, step, width), lambda e, i, p: (e, p[k], first // step + i, 0))

    whole = pl.BlockSpec(sums[0].shape, lambda e, i, p: (0, 0, 0))
    in_specs = [reader(k) for k in range(n)] + [whole] * n
    args = [blocks] * n + list(sums)
    aliases = {}
    if out is not None:
        aliases = {len(args) + 1: 0}
        args.append(out)
        in_specs.append(pl.BlockSpec(memory_space=pltpu.HBM))
    args += after
    in_specs += [pl.BlockSpec(memory_space=pl.ANY)] * len(after)
    peer_shape = jax.ShapeDtypeStruct((experts, count, width), jnp.bfloat16)
    peer_spec = pl.BlockSpec((1, step, width), lambda e, i, p: (e, i, 0))
    own_spec = pl.BlockSpec((1, step, width), lambda e, i, p: (e, first // step + i, p[n]))
    bytes_moved = 6 * n * experts * count * width
    return pl.pallas_call(
        body,
        out_shape=[jax.ShapeDtypeStruct((experts, rows, n * width), jnp.bfloat16)] + [peer_shape] * (n - 1),
        grid_spec=pltpu.PrefetchScalarGridSpec(
            num_scalar_prefetch=1,
            grid=(experts, count // step),
            in_specs=in_specs,
            out_specs=[own_spec] + [peer_spec] * (n - 1),
            scratch_shapes=[pltpu.VMEM((n, count, LANES), jnp.float32)],
        ),
        input_output_aliases=aliases,
        cost_estimate=pl.CostEstimate(flops=bytes_moved, bytes_accessed=bytes_moved, transcendentals=0),
    )(places, *args)


def place(out, pieces, sources, first):
    experts, count, width = pieces[0].shape
    m = len(pieces)

    def body(sources_ref, *refs):
        ins, o = refs[:m], refs[m + 1]
        held, in_sems, out_sems = refs[m + 2 :]
        every = [(k, e) for k in range(m) for e in range(experts)]
        loads = [pltpu.make_async_copy(ins[k].at[e], held.at[k, e], in_sems.at[k, e]) for k, e in every]
        stores = []
        for k, e in every:
            column = pl.multiple_of(sources_ref[k + 1] * width, width)
            target = o.at[e, pl.ds(first, count), pl.ds(column, width)]
            stores.append(pltpu.make_async_copy(held.at[k, e], target, out_sems.at[k, e]))
        for load in loads:
            load.start()
        for load, store in zip(loads, stores):
            load.wait()
            store.start()
        for store in stores:
            store.wait()

    anywhere = pl.BlockSpec(memory_space=pltpu.HBM)
    bytes_moved = 4 * m * experts * count * width
    return pl.pallas_call(
        body,
        out_shape=jax.ShapeDtypeStruct(out.shape, out.dtype),
        grid_spec=pltpu.PrefetchScalarGridSpec(
            num_scalar_prefetch=1,
            grid=(),
            in_specs=[anywhere] * (m + 1),
            out_specs=anywhere,
            scratch_shapes=[
                pltpu.VMEM((m, experts, count, width), jnp.bfloat16),
                pltpu.SemaphoreType.DMA((m, experts)),
                pltpu.SemaphoreType.DMA((m, experts)),
            ],
        ),
        input_output_aliases={m + 1: 0},
        cost_estimate=pl.CostEstimate(flops=bytes_moved, bytes_accessed=bytes_moved, transcendentals=0),
    )(sources, *pieces, out)


def per_device(master_down, router_weight, router_gain):
    n = lax.axis_size("rows")
    me = lax.axis_index("rows")
    experts, total_rows, width = master_down.shape
    rows = total_rows // n
    model = width * n
    groups = plan(rows)
    blocks = master_down.reshape(experts, n, rows, width)
    if n & (n - 1):
        hops = [[(i, (i + k) % n) for i in range(n)] for k in range(n)]
        targets = [(me + k) % n for k in range(n)]
        sources = [(me + n - k) % n for k in range(n)]
    else:
        hops = [[(i, i ^ k) for i in range(n)] for k in range(n)]
        targets = sources = [me ^ k for k in range(n)]
    target_list = jnp.stack(targets + [me]).astype(jnp.int32)
    source_list = target_list if sources is targets else jnp.stack(sources + [me]).astype(jnp.int32)
    far_first = list(range(n - 1, 0, -1))

    def exchange(x):
        got = {k: lax.ppermute(x, "rows", hops[k]) for k in far_first}
        return [x] + [got[k] for k in range(1, n)]

    def local_sums(source, group):
        return jnp.sum(jnp.abs(source[:, :, group[0][0] : sum(group[-1])]), axis=3)

    def shared_sums(g, source):
        sums = local_sums(source, groups[g])
        return exchange(sums)

    out, flying, after, router_rows = None, [], [], None
    serve_router = scale_down = None
    shared = [shared_sums(0, blocks)]
    c, chunks = 0, sum(map(len, groups))
    for g, group in enumerate(groups):
        for i, (first, count) in enumerate(group):
            if c == min(ROUTER_USED, chunks - 1):
                router_rows = lax.optimization_barrier((router_rows, sent[0]))[0]
                ordered = jnp.zeros((n,) + router_rows[0].shape, router_rows[0].dtype)
                for place_of, rows_of in zip(sources, router_rows):
                    ordered = lax.dynamic_update_index_in_dim(ordered, rows_of, place_of, 0)
                row_router = ordered.reshape(n * router_weight.shape[0], router_weight.shape[1])
                serve_router = lax.all_gather(row_router, "owner", axis=1, tiled=True)
                own = [tree_sum(lax.dynamic_index_in_dim(s, me, 1, keepdims=False) for s in sums) for sums in shared]
                scale_down = jnp.concatenate(own, axis=1) / model
                after = [serve_router, scale_down]
            out, *sent = narrow(out, blocks, shared[g], group[0][0], target_list, first, count, after)
            after = []
            if i == min(1, len(group) - 1) and g + 1 < len(groups):
                late = lax.optimization_barrier((blocks, sent[0]))[0]
                shared.append(shared_sums(g + 1, late))
            if c == min(ROUTER_SENT, chunks - 2):
                weight, gain, _ = lax.optimization_barrier((router_weight, router_gain, sent[0]))
                router_rows = exchange((weight * gain[:, None]).astype(jnp.bfloat16))
            got = {k: lax.ppermute(sent[k - 1], "rows", hops[k]) for k in far_first}
            flying.append(([got[k] for k in range(1, n)], first))
            if len(flying) > AHEAD:
                out = place(out, flying[0][0], source_list, flying.pop(0)[1])
            c += 1
    for pieces, first in flying:
        out = place(out, pieces, source_list, first)
    return out, scale_down, serve_router


def solution(mesh):
    return jax.shard_map(
        per_device,
        mesh=mesh,
        in_specs=(P("owner", None, "rows"), P("rows", "owner"), P("rows")),
        out_specs=(P("owner", "rows", None), P("owner", "rows"), P()),
        check_vma=False,
    )
```

```python
import jax
import jax.numpy as jnp
from jax import lax
from jax.experimental import pallas as pl
from jax.experimental.pallas import tpu as pltpu
from jax.sharding import PartitionSpec as P


LANES, TILE, BLOCK = 128, 16, 80
SMALL = 8 << 20
GROUPS = ((4, 3), (3, 9, 8), (10, 10, 10, 10, 10, 9, 7, 4, 3))
TURNS = (1, 2)
AHEAD = 4
ROUTER_SENT, ROUTER_USED = 5, 9
DIRECT = 2
NEAR_DONE = 4


def plan(rows):
    total, at, done, groups = sum(map(sum, GROUPS)), 0, 0, []
    for lengths in GROUPS:
        chunks = []
        for length in lengths:
            done += length
            end = rows if done == total else rows * done // total // TILE * TILE
            if end > at:
                chunks.append((at, end - at))
            at = end
        if chunks:
            groups.append(chunks)
    return groups


def block_of(count):
    return max((u for u in range(TILE, BLOCK + 1, TILE) if count % u == 0), default=count)


def tree_sum(terms):
    terms = list(terms)
    while len(terms) > 1:
        terms = [sum(terms[i + 1 : i + 2], terms[i]) for i in range(0, len(terms), 2)]
    return terms[0]


def narrow(out, blocks, sums, base, places, own, peers, first, count, after):
    experts, n, rows, width = blocks.shape
    model = n * width
    step = block_of(count)
    steps = ([0] if own else []) + list(peers)
    m = len(steps)

    def body(places_ref, *refs):
        ins, sums_refs = refs[:m], refs[m : m + len(sums)]
        outs, factors = refs[-m - 1 : -1], refs[-1]
        e, i = pl.program_id(0), pl.program_id(1)

        @pl.when(i == 0)
        def _():
            inverse = 1.0 / (tree_sum(r[:, first - base : first - base + count] for r in sums_refs) / model)
            row = lax.broadcasted_iota(jnp.int32, inverse.shape, 0)
            for s, k in enumerate(steps):
                chosen = jnp.where(row == e * n + places_ref[k], inverse, 0.0)
                chosen = jnp.sum(chosen, axis=0, keepdims=True)
                factors[s] = jnp.broadcast_to(chosen, (LANES, count)).T

        rows_now = pl.ds(pl.multiple_of(i * step, step), step)
        for s in range(m):
            factor = factors[s, rows_now, :]
            for j in range(0, width, LANES):
                outs[s][0, :, j : j + LANES] = (ins[s][0, 0, :, j : j + LANES] * factor).astype(jnp.bfloat16)

    def reader(k):
        shape = (pl.Element(1), pl.Element(1), pl.Element(step), pl.Element(width))
        return pl.BlockSpec(shape, lambda e, i, p: (e, p[k], pl.multiple_of(first + i * step, TILE), 0))

    whole = pl.BlockSpec(sums[0].shape, lambda e, i, p: (0, 0))
    in_specs = [reader(k) for k in steps] + [whole] * len(sums)
    args = [blocks] * m + list(sums)
    aliases = {}
    if own and out is not None:
        aliases = {len(args) + 1: 0}
        args.append(out)
        in_specs.append(pl.BlockSpec(memory_space=pltpu.HBM))
    args += after
    in_specs += [pl.BlockSpec(memory_space=pl.ANY)] * len(after)
    out_shape = [jax.ShapeDtypeStruct((experts, count, width), jnp.bfloat16)] * len(peers)
    out_specs = [pl.BlockSpec((1, step, width), lambda e, i, p: (e, i, 0))] * len(peers)
    if own:
        out_shape = [jax.ShapeDtypeStruct((experts, rows, n * width), jnp.bfloat16)] + out_shape
        shape = (pl.Element(1), pl.Element(step), pl.Element(width))
        out_specs = [pl.BlockSpec(shape, lambda e, i, p: (e, pl.multiple_of(first + i * step, TILE), pl.multiple_of(p[n] * width, LANES)))] + out_specs
    bytes_moved = 6 * m * experts * count * width
    got = pl.pallas_call(
        body,
        out_shape=out_shape,
        grid_spec=pltpu.PrefetchScalarGridSpec(
            num_scalar_prefetch=1,
            grid=(experts, count // step),
            in_specs=in_specs,
            out_specs=out_specs,
            scratch_shapes=[pltpu.VMEM((m, count, LANES), jnp.float32)],
        ),
        input_output_aliases=aliases,
        compiler_params=pltpu.CompilerParams(vmem_limit_bytes=None if own else SMALL),
        cost_estimate=pl.CostEstimate(flops=bytes_moved, bytes_accessed=bytes_moved, transcendentals=0),
    )(places, *args)
    return (got[0] if own else out), dict(zip(peers, got[-len(peers) :]))


def narrow_opening(parts, sums, places, peers):
    experts, count, width = parts[0].shape
    m, n = len(peers), sums[0].shape[0] // experts

    def body(places_ref, *refs):
        ins, sums_refs, outs = refs[:m], refs[m : m + len(sums)], refs[-m:]
        inverse = 1.0 / (tree_sum(r[:, :count] for r in sums_refs) / (n * width))
        row = lax.broadcasted_iota(jnp.int32, inverse.shape, 0)
        for s, k in enumerate(peers):
            for e in range(experts):
                chosen = jnp.sum(jnp.where(row == e * n + places_ref[k], inverse, 0.0), axis=0, keepdims=True)
                factor = jnp.broadcast_to(chosen, (LANES, count)).T
                for j in range(0, width, LANES):
                    outs[s][e, :, j : j + LANES] = (ins[s][e, :, j : j + LANES] * factor).astype(jnp.bfloat16)

    bytes_moved = 6 * m * experts * count * width
    got = pl.pallas_call(
        body,
        out_shape=[jax.ShapeDtypeStruct((experts, count, width), jnp.bfloat16)] * m,
        grid_spec=pltpu.PrefetchScalarGridSpec(
            num_scalar_prefetch=1,
            grid=(1,),
            in_specs=[pl.BlockSpec(parts[0].shape, lambda i, p: (0, 0, 0))] * m
            + [pl.BlockSpec(sums[0].shape, lambda i, p: (0, 0))] * len(sums),
            out_specs=[pl.BlockSpec(parts[0].shape, lambda i, p: (0, 0, 0))] * m,
        ),
        compiler_params=pltpu.CompilerParams(vmem_limit_bytes=SMALL),
        cost_estimate=pl.CostEstimate(flops=bytes_moved, bytes_accessed=bytes_moved, transcendentals=0),
        name="narrow_opening",
    )(places, *parts, *sums)
    return dict(zip(peers, got))


def place(out, pieces, sources, first, last):
    experts, count, width = pieces[0].shape
    m = len(pieces)

    def body(sources_ref, *refs):
        ins, o = refs[:m], refs[m + 1]
        held, in_sems, out_sems = (ins, None, refs[-1]) if last else refs[m + 2 :]
        every = [(k, e) for k in range(m) for e in range(experts)]
        loads, stores = [], []
        for k, e in every:
            column = pl.multiple_of(sources_ref[k + 1] * width, width)
            target = o.at[e, pl.ds(first, count), pl.ds(column, width)]
            if last:
                stores.append(pltpu.make_async_copy(ins[k].at[e], target, out_sems.at[k, e]))
            else:
                loads.append(pltpu.make_async_copy(ins[k].at[e], held.at[k, e], in_sems.at[k, e]))
                stores.append(pltpu.make_async_copy(held.at[k, e], target, out_sems.at[k, e]))
        for load in loads:
            load.start()
        for s, store in enumerate(stores):
            if loads:
                loads[s].wait()
            store.start()
        for store in stores:
            store.wait()

    anywhere = pl.BlockSpec(memory_space=pltpu.HBM)
    bytes_moved = 4 * m * experts * count * width
    return pl.pallas_call(
        body,
        out_shape=jax.ShapeDtypeStruct(out.shape, out.dtype),
        grid_spec=pltpu.PrefetchScalarGridSpec(
            num_scalar_prefetch=1,
            grid=(),
            in_specs=[pl.BlockSpec(memory_space=pl.ANY) if last else anywhere] * m + [anywhere],
            out_specs=anywhere,
            scratch_shapes=[
                pltpu.VMEM((m, experts, count, width), jnp.bfloat16),
                pltpu.SemaphoreType.DMA((m, experts)),
                pltpu.SemaphoreType.DMA((m, experts)),
            ][2 * last :],
        ),
        input_output_aliases={m + 1: 0},
        compiler_params=pltpu.CompilerParams(vmem_limit_bytes=SMALL if last else None),
        cost_estimate=pl.CostEstimate(flops=bytes_moved, bytes_accessed=bytes_moved, transcendentals=0),
    )(sources, *pieces, out)


def per_device(master_down, router_weight, router_gain):
    n = lax.axis_size("rows")
    me = lax.axis_index("rows")
    experts, total_rows, width = master_down.shape
    rows = total_rows // n
    model = width * n
    groups = plan(rows)
    blocks = master_down.reshape(experts, n, rows, width)
    if n & (n - 1):
        hops = [[(i, (i + k) % n) for i in range(n)] for k in range(n)]
        targets = [(me + k) % n for k in range(n)]
        sources = [(me + n - k) % n for k in range(n)]
    else:
        hops = [[(i, i ^ k) for i in range(n)] for k in range(n)]
        targets = sources = [me ^ k for k in range(n)]
    target_list = jnp.stack(targets + [me]).astype(jnp.int32)
    source_list = target_list if sources is targets else jnp.stack(sources + [me]).astype(jnp.int32)
    paired = n % 2 == 0 and not n & (n - 1)
    near = [1] if paired else []
    far = [k for k in range(n - 1, 0, -1) if k not in near]

    def exchange(x, ks):
        return {k: lax.ppermute(x, "rows", hops[k]) for k in ks}

    def shared_sums(g, source):
        lo, hi = groups[g][0][0], sum(groups[g][-1])
        flat = source.reshape(experts * n, rows, width)
        sums = jnp.sum(jnp.abs(flat[:, lo:hi]), axis=2)
        if paired and g and g == len(groups) - 1:
            pair = sums + exchange(sums, near)[1]
            got = exchange(pair, [k for k in far if k % 2 == 0])
            return [pair] + [got[k] for k in sorted(got)]
        got = exchange(sums, far + near)
        return [sums] + [got[k] for k in range(1, n)]

    def send(pieces, ks):
        return {k: lax.ppermute(pieces[k], "rows", hops[k]) for k in ks}

    out, flying, after, router_rows = None, [], [], None
    serve_router = scale_down = None
    shared = [shared_sums(0, blocks)]
    c, chunks = 0, sum(map(len, groups))
    for g, group in enumerate(groups):
        base = group[0][0]
        turn = min(TURNS[g], len(group) - 1) if g + 1 < len(groups) else None
        for i, (first, count) in enumerate(group):
            if c == min(ROUTER_USED, chunks - 1):
                router_rows = lax.optimization_barrier((router_rows, token))[0]
                ordered = jnp.zeros((n,) + router_rows[0].shape, router_rows[0].dtype)
                for k in range(n):
                    ordered = lax.dynamic_update_index_in_dim(ordered, router_rows[k], sources[k], 0)
                row_router = ordered.reshape(n * router_weight.shape[0], router_weight.shape[1])
                serve_router = lax.all_gather(row_router, "owner", axis=1, tiled=True)
                totals = [tree_sum(s).reshape(experts, n, -1) for s in shared]
                totals = [lax.dynamic_index_in_dim(t, me, 1, keepdims=False) for t in totals]
                scale_down = jnp.concatenate(totals, axis=1) / model
                after = [serve_router, scale_down]
            opening = c == 0 and bool(far) and chunks > NEAR_DONE
            if opening:
                source = lax.optimization_barrier((blocks, shared[0][0]))[0]
                starts = [(0, targets[k], first, 0) for k in far]
                parts = [lax.dynamic_slice(source, s, (experts, 1, count, width))[:, 0] for s in starts]
                pieces = narrow_opening(lax.optimization_barrier(parts), shared[0], target_list, far)
            else:
                out, pieces = narrow(out, blocks, shared[g], base, target_list, True, far + near, first, count, after)
            after, token = [], pieces[(far + near)[0]]
            if i == turn:
                shared.append(shared_sums(g + 1, lax.optimization_barrier((blocks, token))[0]))
            if c == min(ROUTER_SENT, chunks - 2):
                weight, gain, _ = lax.optimization_barrier((router_weight, router_gain, token))
                part = (weight * gain[:, None]).astype(jnp.bfloat16)
                got = exchange(part, far + near)
                router_rows = [part] + [got[k] for k in range(1, n)]
            flying.append((send(pieces, far if opening else far + near), first))
            if c == NEAR_DONE and len(flying[0][0]) < n - 1:
                out, pieces = narrow(
                    out, blocks, shared[0], 0, target_list, True, near, groups[0][0][0], groups[0][0][1], []
                )
                flying[0][0].update(send(pieces, near))
            if len(flying) > AHEAD:
                got, at = flying.pop(0)
                out = place(out, [got[k] for k in range(1, n)], source_list, at, False)
            c += 1
    while flying:
        got, at = flying.pop(0)
        out = place(out, [got[k] for k in range(1, n)], source_list, at, len(flying) < DIRECT)
    return out, scale_down, serve_router


def solution(mesh):
    return jax.shard_map(
        per_device,
        mesh=mesh,
        in_specs=(P("owner", None, "rows"), P("rows", "owner"), P("rows")),
        out_specs=(P("owner", "rows", None), P("owner", "rows"), P()),
        check_vma=False,
    )
```
